32 devices in a mesh: dp: 8 (over z, x), mp: 4 (over y, core).
Axes of the slice: x: 2, y: 2, z: 4, core: 2. Of those that a mesh axis runs over, the one named last changes fastest.
Arguments:
- queries: bfloat16 [16, 16, 5120], P('dp', None, 'mp')
- key_value_cache: bfloat16 [128, 2, 128, 1024], P('dp', None, None, 'mp'), may hold values from -6 to 6
- slot_tags: int32 [128], P('dp'), may hold values from 0 to 15, as said below
- span_key_value: bfloat16 [16, 2, 16, 1024], P('dp', None, None, 'mp'), may hold values from -6 to 6
- answer_id: int32 [16], P('dp'), may hold values from 0 to 127
- w_cand: bfloat16 [5120, 128], P('mp')
Outputs:
- attended: bfloat16 [16, 16, 5120], P('dp', None, 'mp')
- chain_score: float32 [16], P('dp')
- answer_tally: float32 [1, 128], P(None, 'dp')
The draws below stay inside these ranges and needn't reach their ends.
Inputs may be any that keep to these rules, and one draw needn't show every extreme that they name: `slot_tags`: among the 16 blocks of any one index of dp, at most 2 belong to the chains o * 2 to o * 2 + 1 of any one o, and for some o every index of dp holds exactly 2 such blocks. A chain may have no cached block.
All inputs are finite; a program needn't handle non-finite values.
Results may differ from the reference program's by a relative error of at most 0.0075.
Values may be sent and summed in bfloat16 or wider, within the bound.
No kernel may reach another device: no remote copies, remote signals or barrier semaphores. Data moves between devices by JAX's collectives and lax.ppermute only.
A program may use at most 128 MiB of HBM per device.

```python
import jax
import jax.numpy as jnp
from jax import lax

QUERY_HEADS = 40
KEY_VALUE_HEADS = 8
HEAD_SIZE = 128
NCAND = 128
BLOCK_TOKENS = 128
ANSWER_TOKENS = 16
PEER = 2
SAMPLES = 16
CH_DEV = 2
SLOTS = 16
CHAIN_COUNT = 16
TOTAL_BLOCKS = 128


def draw_queries(key, part):
    first = jax.random.fold_in(key, 0)
    base = jax.random.normal(first, (CHAIN_COUNT, ANSWER_TOKENS, QUERY_HEADS * HEAD_SIZE), jnp.float32)
    return base.astype(jnp.bfloat16)


def draw_w_cand(key, part):
    first = jax.random.fold_in(key, 0)
    base = jax.random.normal(first, (QUERY_HEADS * HEAD_SIZE, NCAND), jnp.float32) * (8.0 / (QUERY_HEADS * HEAD_SIZE) ** 0.5)
    return base.astype(jnp.bfloat16)


def draw_slot_tags(key, part):
    lookup_matrix = jax.random.split(jax.random.fold_in(key, 7), 5)
    accelerator_roster = CHAIN_COUNT // CH_DEV
    couple_sequence = accelerator_roster * PEER
    extra_credit = jax.random.randint(lookup_matrix[0], (accelerator_roster,), 0, 3)
    selected_reply = jax.random.randint(lookup_matrix[1], (), 0, accelerator_roster)
    extra_credit = jnp.where(jnp.arange(accelerator_roster) == selected_reply, 3, extra_credit)
    random_perturbation = jax.random.randint(lookup_matrix[2], (accelerator_roster, couple_sequence), 0, 4096)
    couple_container = jnp.arange(couple_sequence) // PEER
    sorted_permutation = (extra_credit[couple_container][None, :] * 4096 + random_perturbation) * couple_sequence + jnp.arange(couple_sequence)[None, :]
    order = jnp.argsort(-sorted_permutation, axis=1, stable=True)[:, :SLOTS]
    owners_of = order // PEER
    chain_pick = jax.random.randint(lookup_matrix[3], (accelerator_roster, SLOTS), 0, CH_DEV)
    tags_grid = owners_of * CH_DEV + chain_pick
    mixing = jax.random.randint(lookup_matrix[4], (accelerator_roster, SLOTS), 0, 1 << 20) * SLOTS + jnp.arange(SLOTS)[None, :]
    shuffle = jnp.argsort(mixing, axis=1, stable=True)
    tags_grid = jnp.take_along_axis(tags_grid, shuffle, axis=1)
    return tags_grid.reshape(accelerator_roster * SLOTS).astype(jnp.int32)


def place_ends(result, stream_key, smallest, top_value):
    longest = result.shape.index(max(result.shape))
    spots = []
    for shift in (0, 1):
        where = [jax.random.randint(jax.random.fold_in(stream_key, axis), (), 0, length) for axis, length in enumerate(result.shape)]
        where[longest] = (where[longest] + shift) % result.shape[longest]
        spots.append(tuple(where))
    return result.at[spots[0]].set(smallest).at[spots[1]].set(top_value)


def shard_levels(rng, extent, cuts, least, high):
    factor_of = 1.0
    for dim, blocks in cuts:
        steps = jax.random.uniform(jax.random.fold_in(jax.random.fold_in(rng, 6), dim), (blocks,), jnp.float32, least / len(cuts), high / len(cuts))
        factor_of = factor_of * jnp.repeat(jnp.exp(steps), extent[dim] // blocks).reshape((-1,) + (1,) * (len(extent) - 1 - dim))
    return factor_of


def bell_draw(rng, dims, deviation, bound, shards=(), kind=jnp.bfloat16):
    result = deviation * jax.random.normal(rng, dims, jnp.float32)
    if shards:
        result = result * shard_levels(rng, dims, shards, -0.22, 0.18)
    return jnp.clip(result, -bound, bound).astype(kind)


def setup_inputs(seed: int = 0) -> dict:
    seeds = jax.random.split(jax.random.key(seed), 7)
    queries = draw_queries(jax.random.fold_in(seeds[6], 71), 0)
    key_value_cache = bell_draw(seeds[1], (TOTAL_BLOCKS, 2, BLOCK_TOKENS, KEY_VALUE_HEADS * HEAD_SIZE), 1.0, 6.0, ((0, 8), (3, 4)))
    slot_tags = draw_slot_tags(jax.random.fold_in(seeds[6], 71), 0)
    span_key_value = bell_draw(seeds[3], (CHAIN_COUNT, 2, ANSWER_TOKENS, KEY_VALUE_HEADS * HEAD_SIZE), 1.0, 6.0, ((0, 8), (3, 4)))
    answer_id = place_ends(jax.random.randint(seeds[4], (CHAIN_COUNT,), 0, NCAND), jax.random.fold_in(seeds[4], 1), 0, NCAND - 1).astype(jnp.int32)
    w_cand = draw_w_cand(jax.random.fold_in(seeds[6], 71), 0)
    return {"queries": queries, "key_value_cache": key_value_cache, "slot_tags": slot_tags, "span_key_value": span_key_value, "answer_id": answer_id, "w_cand": w_cand}


big_neg = -1e30


def span_terms(single_queries, single_span):
    head_group = QUERY_HEADS // KEY_VALUE_HEADS
    query_rows = single_queries.astype(jnp.float32).reshape(ANSWER_TOKENS, KEY_VALUE_HEADS, head_group, HEAD_SIZE)
    lookup_matrix = single_span[0].astype(jnp.float32).reshape(ANSWER_TOKENS, KEY_VALUE_HEADS, HEAD_SIZE)
    value_rows = single_span[1].astype(jnp.float32).reshape(ANSWER_TOKENS, KEY_VALUE_HEADS, HEAD_SIZE)
    logit_rows = jnp.einsum('qufe,xue->ufqx', query_rows, lookup_matrix) * (HEAD_SIZE ** -0.5)
    causal = jnp.arange(ANSWER_TOKENS)[:, None] >= jnp.arange(ANSWER_TOKENS)[None, :]
    logit_rows = jnp.where(causal, logit_rows, big_neg)
    peak = jnp.max(logit_rows, axis=-1)
    weights = jnp.exp(logit_rows - peak[..., None])
    total = jnp.sum(weights, axis=-1)
    rounded_scores = lax.optimization_barrier(weights.astype(jnp.bfloat16))
    summed_scores = jnp.einsum('wefs,swn->wefn', rounded_scores.astype(jnp.float32), value_rows)
    return peak, total, summed_scores


def reference(queries, key_value_cache, slot_tags, span_key_value, answer_id, w_cand):
    head_group = QUERY_HEADS // KEY_VALUE_HEADS
    chains_all = queries.shape[0]
    peak, total, summed_scores = jax.vmap(span_terms)(queries, span_key_value)

    def absorb(carry, item):
        peak, total, summed_scores = carry
        current_tag, block_entry = item
        query_rows = queries[current_tag].astype(jnp.float32).reshape(ANSWER_TOKENS, KEY_VALUE_HEADS, head_group, HEAD_SIZE)
        lookup_matrix = block_entry[0].astype(jnp.float32).reshape(BLOCK_TOKENS, KEY_VALUE_HEADS, HEAD_SIZE)
        value_rows = block_entry[1].astype(jnp.float32).reshape(BLOCK_TOKENS, KEY_VALUE_HEADS, HEAD_SIZE)
        logit_rows = jnp.einsum('qufe,xue->ufqx', query_rows, lookup_matrix) * (HEAD_SIZE ** -0.5)
        older = peak[current_tag]
        fresh = jnp.maximum(older, jnp.max(logit_rows, axis=-1))
        weights = jnp.exp(logit_rows - fresh[..., None])
        shrink = jnp.exp(older - fresh)
        rounded_scores = lax.optimization_barrier(weights.astype(jnp.bfloat16))
        added_terms = jnp.einsum('wefs,swn->wefn', rounded_scores.astype(jnp.float32), value_rows)
        total = total.at[current_tag].set(total[current_tag] * shrink + jnp.sum(weights, axis=-1))
        summed_scores = summed_scores.at[current_tag].set(summed_scores[current_tag] * shrink[..., None] + added_terms)
        peak = peak.at[current_tag].set(fresh)
        return (peak, total, summed_scores), None

    (peak, total, summed_scores), _ = lax.scan(absorb, (peak, total, summed_scores), (slot_tags, key_value_cache))
    output = summed_scores / total[..., None]
    output = jnp.transpose(output, (0, 3, 1, 2, 4)).reshape(chains_all, ANSWER_TOKENS, QUERY_HEADS * HEAD_SIZE)
    attended = output.astype(jnp.bfloat16)
    logit_rows = jnp.dot(attended.reshape(chains_all * ANSWER_TOKENS, QUERY_HEADS * HEAD_SIZE), w_cand, preferred_element_type=jnp.float32)
    logit_rows = logit_rows.reshape(chains_all, ANSWER_TOKENS, NCAND)
    top_logit = jnp.max(logit_rows, axis=-1, keepdims=True)
    log_norm = top_logit[..., 0] + jnp.log(jnp.sum(jnp.exp(logit_rows - top_logit), axis=-1))
    answer_hot = (answer_id[:, None] == jnp.arange(NCAND, dtype=jnp.int32)[None, :]).astype(jnp.float32)
    picked = jnp.sum(logit_rows * answer_hot[:, None, :], axis=-1)
    chain_score = jnp.mean(picked - log_norm, axis=-1)
    prompt_of = jnp.arange(chains_all, dtype=jnp.int32) // SAMPLES
    prompt_hot = (prompt_of[:, None] == jnp.arange(chains_all // SAMPLES, dtype=jnp.int32)[None, :]).astype(jnp.float32)
    answer_tally = jnp.dot(prompt_hot.T, chain_score[:, None] * answer_hot, precision=lax.Precision.HIGHEST)
    return attended, chain_score, answer_tally
```

```python
import jax
import jax.numpy as jnp
from jax import lax
from jax.sharding import PartitionSpec as P

QUERY_HEADS = 40
KEY_VALUE_HEADS = 8
HEAD_SIZE = 128
NCAND = 128
PEER = 2
SAMPLES = 16


big_neg = -1e30


def block_terms(picked, blocks, causal):
    count = picked.shape[0]
    span = picked.shape[1]
    width = blocks.shape[2]
    heads_kv = blocks.shape[3] // HEAD_SIZE
    head_group = QUERY_HEADS // KEY_VALUE_HEADS
    query_rows = picked.reshape(count, span, heads_kv, head_group, HEAD_SIZE)
    lookup_matrix = blocks[:, 0].reshape(count, width, heads_kv, HEAD_SIZE)
    value_rows = blocks[:, 1].reshape(count, width, heads_kv, HEAD_SIZE)
    logit_rows = jnp.einsum(
        "nakgd,nbkd->nkgab", query_rows, lookup_matrix, preferred_element_type=jnp.float32
    ) * HEAD_SIZE ** (-0.5)
    if causal:
        allowed = jnp.arange(span)[:, None] >= jnp.arange(width)[None, :]
        logit_rows = jnp.where(allowed, logit_rows, big_neg)
    peaks = jnp.max(logit_rows, axis=-1)
    weights = jnp.exp(logit_rows - peaks[..., None])
    totals = jnp.sum(weights, axis=-1)
    summed_scores = jnp.einsum(
        "nkgab,nbkd->nkgad",
        weights.astype(jnp.bfloat16),
        value_rows,
        preferred_element_type=jnp.float32,
    )
    return (peaks, totals, summed_scores)


def merge_items(peaks, totals, summed_scores, member):
    member_f = member.astype(jnp.float32)
    masked = jnp.where(member[:, :, None, None, None], peaks[:, None], big_neg)
    chain_peak = jnp.max(masked, axis=0)
    item_peak = jnp.einsum("nc,ckga->nkga", member_f, chain_peak, precision=lax.Precision.HIGHEST)
    present = jnp.any(member, axis=1)
    factor = jnp.where(present[:, None, None, None], jnp.exp(peaks - item_peak), 0.0)
    chain_total = jnp.einsum(
        "nc,nkga->ckga", member_f, totals * factor, precision=lax.Precision.HIGHEST
    )
    chain_sum = jnp.einsum(
        "nc,nkgad->ckgad",
        member_f,
        summed_scores * factor[..., None],
        precision=lax.Precision.HIGHEST,
    )
    return (chain_peak, chain_total, chain_sum)


def fold_pair(first, second):
    overall = jnp.maximum(first[0], second[0])
    left = jnp.exp(first[0] - overall)
    right = jnp.exp(second[0] - overall)
    total = first[1] * left + second[1] * right
    summed_scores = first[2] * left[..., None] + second[2] * right[..., None]
    return (overall, total, summed_scores)


def per_device(queries, key_value_cache, slot_tags, span_key_value, answer_id, w_cand):
    accelerator_roster = lax.axis_size("dp")
    position = lax.axis_index("dp")
    chains_here = queries.shape[0]
    features = queries.shape[2]
    slots_here = slot_tags.shape[0]
    owner_index = slot_tags // chains_here
    chain_local = slot_tags % chains_here
    owner_hot = (
        owner_index[:, None] == jnp.arange(accelerator_roster, dtype=jnp.int32)[None, :]
    ).astype(jnp.int32)
    running = jnp.cumsum(owner_hot, axis=0) - 1
    rank_in = jnp.sum(owner_hot * running, axis=1)
    target = owner_index * PEER + rank_in
    places_all = accelerator_roster * PEER
    hit = (target[:, None] == jnp.arange(places_all, dtype=jnp.int32)[None, :]).astype(jnp.int32)
    source_row = jnp.sum(hit * jnp.arange(slots_here, dtype=jnp.int32)[:, None], axis=0)
    is_filled = jnp.sum(hit, axis=0) > 0
    send_chain = jnp.where(is_filled, jnp.sum(hit * chain_local[:, None], axis=0), chains_here)
    send_blocks = key_value_cache[source_row].reshape(
        (accelerator_roster, PEER) + key_value_cache.shape[1:]
    )
    send_chain = send_chain.reshape(accelerator_roster, PEER)
    blocks = lax.all_to_all(send_blocks, "dp", split_axis=0, concat_axis=0, tiled=True)
    places = lax.all_to_all(send_chain, "dp", split_axis=0, concat_axis=0, tiled=True)
    count = places.shape[0] * places.shape[1]
    flat_places = places.reshape(count)
    picked = queries[jnp.clip(flat_places, 0, chains_here - 1)]
    peaks, totals, summed_scores = block_terms(
        picked, blocks.reshape((count,) + blocks.shape[2:]), False
    )
    lead = places.shape
    peaks, totals, summed_scores, places = (
        peaks.reshape(lead + peaks.shape[1:]),
        totals.reshape(lead + totals.shape[1:]),
        summed_scores.reshape(lead + summed_scores.shape[1:]),
        places,
    )
    count = places.shape[0] * places.shape[1]
    member = places.reshape(count)[:, None] == jnp.arange(chains_here, dtype=jnp.int32)[None, :]
    remote = merge_items(
        peaks.reshape((count,) + peaks.shape[2:]),
        totals.reshape((count,) + totals.shape[2:]),
        summed_scores.reshape((count,) + summed_scores.shape[2:]),
        member,
    )
    own_span = block_terms(queries, span_key_value, True)
    final_peak, final_total, final_sum = fold_pair(own_span, remote)
    output = final_sum / final_total[..., None]
    output = jnp.transpose(output, (0, 3, 1, 2, 4)).reshape(chains_here, queries.shape[1], features)
    attended = output.astype(jnp.bfloat16)
    span = queries.shape[1]
    partial_logits = jnp.dot(
        attended.reshape(chains_here * span, features), w_cand, preferred_element_type=jnp.float32
    )
    gathered = lax.all_gather(partial_logits, "mp")
    logit_rows = jnp.sum(gathered, axis=0).reshape(chains_here, span, NCAND)
    top_logit = jnp.max(logit_rows, axis=-1, keepdims=True)
    log_norm = top_logit[..., 0] + jnp.log(jnp.sum(jnp.exp(logit_rows - top_logit), axis=-1))
    answer_hot = (answer_id[:, None] == jnp.arange(NCAND, dtype=jnp.int32)[None, :]).astype(
        jnp.float32
    )
    chosen_logit = jnp.sum(logit_rows * answer_hot[:, None, :], axis=-1)
    chain_score = jnp.mean(chosen_logit - log_norm, axis=-1)
    prompt_count = accelerator_roster * chains_here // SAMPLES
    global_chain = position * chains_here + jnp.arange(chains_here, dtype=jnp.int32)
    prompt_hot = (
        (global_chain // SAMPLES)[:, None] == jnp.arange(prompt_count, dtype=jnp.int32)[None, :]
    ).astype(jnp.float32)
    tally_terms = jnp.dot(
        prompt_hot.T, chain_score[:, None] * answer_hot, precision=lax.Precision.HIGHEST
    )
    step = 1
    while step < accelerator_roster:
        pairs = [(i, i ^ step) for i in range(accelerator_roster)]
        tally_terms = tally_terms + lax.ppermute(tally_terms, "dp", pairs)
        step *= 2
    per = NCAND // accelerator_roster
    answer_tally = lax.dynamic_slice_in_dim(tally_terms, position * per, per, axis=1)
    return (attended, chain_score, answer_tally)


def solution(mesh):
    in_specs = (
        P("dp", None, "mp"),
        P("dp", None, None, "mp"),
        P("dp"),
        P("dp", None, None, "mp"),
        P("dp"),
        P("mp", None),
    )
    out_specs = (P("dp", None, "mp"), P("dp"), P(None, "dp"))
    return jax.shard_map(
        per_device, mesh=mesh, in_specs=in_specs, out_specs=out_specs, check_vma=False
    )
```

```python
import functools

import jax
import jax.numpy as jnp
from jax import lax
from jax.experimental import pallas as pl
from jax.experimental.pallas import tpu as pltpu
from jax.sharding import PartitionSpec as P

QUERY_HEADS = 40
KEY_VALUE_HEADS = 8
HEAD_SIZE = 128
NCAND = 128
PEER = 2
SAMPLES = 16
GROUP = QUERY_HEADS // KEY_VALUE_HEADS
LANES = 128
TEAM = 4
BIG_NEG = -1e30


VMEM = pltpu.VMEM
F32 = jnp.float32
BF16 = jnp.bfloat16


def params(mib=48):
    return pltpu.CompilerParams(vmem_limit_bytes=mib * 1024 * 1024)


def round16(count):
    return (count + 15) // 16 * 16


def note_rows(count):
    return round16(count)


def find_slots(tags_ref, slot_ref, count_ref, chains_here, owners):
    def clear(o, _):
        count_ref[o] = 0
        for k in range(PEER):
            slot_ref[o * PEER + k] = -1
        return 0

    lax.fori_loop(0, owners, clear, 0)

    def place(s, _):
        owner = tags_ref[s] // chains_here
        rank = jnp.minimum(count_ref[owner], PEER - 1)
        slot_ref[owner * PEER + rank] = s
        count_ref[owner] = rank + 1
        return 0

    lax.fori_loop(0, tags_ref.shape[0], place, 0)


def pack_kernel(jobs, chains_here, owners, place_ref, tags_ref, cache_ref, *refs):
    outs = refs[: len(jobs)]
    slot_ref, count_ref, sem = refs[len(jobs) :]
    width = cache_ref.shape[2]
    row, high, high_count = place_ref[0], place_ref[1], owners // TEAM
    find_slots(tags_ref, slot_ref, count_ref, chains_here, owners)
    copies = []
    for out, (offset, first, classes) in zip(outs, jobs):
        member = row ^ offset
        blocks = classes * PEER
        note = jnp.full((note_rows(blocks), out.shape[1]), float(chains_here), F32)
        line = lax.broadcasted_iota(jnp.int32, note.shape, 0)
        for h in range(classes):
            owner = lax.rem(high + first + h, high_count) * TEAM + member
            for k in range(PEER):
                slot = slot_ref[owner * PEER + k]
                safe = jnp.maximum(slot, 0)
                chain = jnp.where(slot < 0, chains_here, tags_ref[safe] % chains_here)
                index = h * PEER + k
                for part in range(2):
                    copy = pltpu.make_async_copy(
                        cache_ref.at[safe, part],
                        out.at[pl.ds((index * 2 + part) * width, width)],
                        sem.at[len(copies)],
                    )
                    copy.start()
                    copies.append(copy)
                note = jnp.where(line == index, chain.astype(F32), note)
        out[pl.ds(blocks * 2 * width, note_rows(blocks)), :] = note.astype(BF16)
    for copy in copies:
        copy.wait()


def pack(jobs, chains_here, owners, place, tags, cache):
    width, lanes = cache.shape[2], cache.shape[3]
    shapes = []
    for _, _, classes in jobs:
        blocks = classes * PEER
        shapes.append(jax.ShapeDtypeStruct((blocks * 2 * width + note_rows(blocks), lanes), BF16))
    moved = sum(s.shape[0] * s.shape[1] * 2 for s in shapes)
    count = sum(classes * PEER * 2 for _, _, classes in jobs)
    return pl.pallas_call(
        functools.partial(pack_kernel, jobs, chains_here, owners),
        out_shape=tuple(shapes),
        in_specs=[
            pl.BlockSpec(memory_space=pltpu.SMEM),
            pl.BlockSpec(memory_space=pltpu.SMEM),
            pl.BlockSpec(memory_space=pl.ANY),
        ],
        out_specs=tuple(pl.BlockSpec(memory_space=VMEM) for _ in jobs),
        scratch_shapes=[
            pltpu.SMEM((owners * PEER,), jnp.int32),
            pltpu.SMEM((owners,), jnp.int32),
            pltpu.SemaphoreType.DMA((count,)),
        ],
        compiler_params=params(),
        cost_estimate=pl.CostEstimate(flops=0, bytes_accessed=2 * moved, transcendentals=0),
    )(place, tags, cache)


def query_rows(q_ref, lead, g):
    chains = q_ref.shape[-3]
    tiles = []
    for c in range(chains):
        for j in range(GROUP):
            at = (g * GROUP + j) * HEAD_SIZE
            tiles.append(q_ref[lead + (c, slice(None), pl.ds(at, HEAD_SIZE))])
    return jnp.concatenate(tiles, axis=0)


def dot_nt(a, b):
    return lax.dot_general(a, b, (((1,), (1,)), ((), ())), preferred_element_type=F32)


def block_tiles(sources, h, classes, g, queries, chain_of_row, width):
    scale = HEAD_SIZE**-0.5
    tiles = []
    for source in sources:
        notes = source[pl.ds(classes * PEER * 2 * width, note_rows(classes * PEER)), pl.ds(0, width)].astype(F32)
        for k in range(PEER):
            index = h * PEER + k
            keys = source[pl.ds(index * 2 * width, width), pl.ds(g * HEAD_SIZE, HEAD_SIZE)]
            values = source[pl.ds((index * 2 + 1) * width, width), pl.ds(g * HEAD_SIZE, HEAD_SIZE)]
            valid = notes[index : index + 1, :] == chain_of_row
            scores = jnp.where(valid, dot_nt(queries, keys) * scale, BIG_NEG)
            tiles.append((scores, valid, values))
    return tiles


def reduce_tiles(tiles):
    peak = functools.reduce(jnp.maximum, [jnp.max(s, axis=1, keepdims=True) for s, _, _ in tiles])
    total, summed = None, None
    for scores, valid, values in tiles:
        weights = jnp.where(valid, jnp.exp(scores - peak), 0.0)
        part = jnp.sum(weights, axis=1, keepdims=True)
        added = jnp.dot(weights.astype(BF16), values, preferred_element_type=F32)
        total = part if total is None else total + part
        summed = added if summed is None else summed + added
    return peak, total, summed


def diagonal(rows):
    return lax.broadcasted_iota(jnp.int32, (rows, LANES), 0) == lax.broadcasted_iota(jnp.int32, (rows, LANES), 1)


def pieces_of(rows):
    return [(at, min(LANES, rows - at)) for at in range(0, rows, LANES)]


def fold_kernel(classes, width, place_ref, *refs):
    q_refs, sources, out_refs = refs[:classes], refs[classes : classes + TEAM], refs[classes + TEAM :]
    chains, span = q_refs[0].shape[0], q_refs[0].shape[1]
    rows = chains * GROUP * span
    heads = q_refs[0].shape[2] // HEAD_SIZE // GROUP
    chain_of_row = (lax.broadcasted_iota(jnp.int32, (rows, width), 0) // (GROUP * span)).astype(F32)
    cuts = pieces_of(rows)
    for h in range(classes):
        out_ref = out_refs[h]
        line = lax.broadcasted_iota(jnp.int32, (out_ref.shape[0] - heads * rows, LANES), 0)
        tail = jnp.zeros(line.shape, F32)
        for g in range(heads):
            queries = query_rows(q_refs[h], (), g)
            peak, total, summed = reduce_tiles(
                block_tiles(sources, h, classes, g, queries, chain_of_row, width)
            )
            empty = total <= 0.0
            safe = jnp.where(empty, 1.0, total)
            out_ref[pl.ds(g * rows, rows), :] = (summed / safe).astype(BF16)
            logs = jnp.where(empty, BIG_NEG, peak + jnp.log(safe))
            for i, (at, size) in enumerate(cuts):
                flat = jnp.sum(
                    jnp.where(diagonal(size), logs[at : at + size, :], 0.0), axis=0, keepdims=True
                )
                first = flat.astype(BF16).astype(F32)
                rest = flat - first
                second = rest.astype(BF16).astype(F32)
                third = rest - second
                for p, piece in enumerate((first, second, third)):
                    at_line = (p * heads + g) * len(cuts) + i
                    tail = jnp.where(line == at_line, piece, tail)
        out_ref[pl.ds(heads * rows, line.shape[0]), :] = tail.astype(BF16)


def message_rows(rows, heads):
    return heads * rows + round16(3 * heads * len(pieces_of(rows)))


def fold(queries, sources, width, place):
    classes = len(queries)
    chains, span, features = queries[0].shape
    rows, heads = chains * GROUP * span, features // HEAD_SIZE // GROUP
    flops = 4 * classes * heads * rows * TEAM * PEER * width * HEAD_SIZE
    return pl.pallas_call(
        functools.partial(fold_kernel, classes, width),
        out_shape=tuple(
            jax.ShapeDtypeStruct((message_rows(rows, heads), LANES), BF16) for _ in range(classes)
        ),
        in_specs=[pl.BlockSpec(memory_space=pltpu.SMEM)]
        + [pl.BlockSpec(memory_space=VMEM)] * (classes + TEAM),
        out_specs=tuple(pl.BlockSpec(memory_space=VMEM) for _ in range(classes)),
        compiler_params=params(),
        cost_estimate=pl.CostEstimate(flops=flops, bytes_accessed=1 << 20, transcendentals=0),
    )(place, *queries, *sources)


def finish_kernel(classes, width, *refs):
    q_ref, span_ref, w_ref = refs[:3]
    sources = refs[3 : 3 + TEAM]
    partials = refs[3 + TEAM : 3 + TEAM + classes]
    attended_ref, logits_ref = refs[3 + TEAM + classes :]
    chains, span = q_ref.shape[0], q_ref.shape[1]
    rows = chains * GROUP * span
    heads = q_ref.shape[2] // HEAD_SIZE // GROUP
    scale = HEAD_SIZE**-0.5
    chain_of_row = (lax.broadcasted_iota(jnp.int32, (rows, width), 0) // (GROUP * span)).astype(F32)
    shape = (rows, chains * span)
    row, key = lax.broadcasted_iota(jnp.int32, shape, 0), lax.broadcasted_iota(jnp.int32, shape, 1)
    causal = (row // (GROUP * span) == key // span) & (row % span >= key % span)
    cuts = pieces_of(rows)
    logits = jnp.zeros(logits_ref.shape, F32)
    for g in range(heads):
        queries = query_rows(q_ref, (), g)
        tiles = block_tiles(sources, 0, 1, g, queries, chain_of_row, width)
        lanes = pl.ds(g * HEAD_SIZE, HEAD_SIZE)
        keys = jnp.concatenate([span_ref[c, 0, :, lanes] for c in range(chains)], axis=0)
        values = jnp.concatenate([span_ref[c, 1, :, lanes] for c in range(chains)], axis=0)
        scores = jnp.where(causal, dot_nt(queries, keys) * scale, BIG_NEG)
        tiles.append((scores, causal, values))
        peak, total, summed = reduce_tiles(tiles)
        for partial in partials:
            tail = partial[pl.ds(heads * rows, partial.shape[0] - heads * rows), :].astype(F32)
            columns = []
            for i, (at, size) in enumerate(cuts):
                lines = [(p * heads + g) * len(cuts) + i for p in range(3)]
                flat = sum(tail[n : n + 1, :] for n in lines)
                columns.append(jnp.sum(jnp.where(diagonal(size), flat, 0.0), axis=1, keepdims=True))
            logs = jnp.concatenate(columns, axis=0)
            best = jnp.maximum(peak, logs)
            left, right = jnp.exp(peak - best), jnp.exp(logs - best)
            other = partial[pl.ds(g * rows, rows), :].astype(F32)
            summed = summed * left + other * right
            total = total * left + right
            peak = best
        result = (summed / total).astype(BF16)
        for j in range(GROUP):
            at = (g * GROUP + j) * HEAD_SIZE
            picked = []
            for c in range(chains):
                part = result[(c * GROUP + j) * span : (c * GROUP + j + 1) * span, :]
                attended_ref[c, :, pl.ds(at, HEAD_SIZE)] = part
                picked.append(part)
            logits = logits + jnp.dot(
                jnp.concatenate(picked, axis=0),
                w_ref[pl.ds(at, HEAD_SIZE), :],
                preferred_element_type=F32,
            )
    logits_ref[...] = logits


def finish(queries, span_key_value, w_cand, sources, partials, width):
    chains, span, _ = queries.shape
    return pl.pallas_call(
        functools.partial(finish_kernel, len(partials), width),
        out_shape=(
            jax.ShapeDtypeStruct(queries.shape, BF16),
            jax.ShapeDtypeStruct((chains * span, NCAND), F32),
        ),
        in_specs=[pl.BlockSpec(memory_space=VMEM)] * (3 + TEAM + len(partials)),
        out_specs=(pl.BlockSpec(memory_space=VMEM),) * 2,
        compiler_params=params(),
        cost_estimate=pl.CostEstimate(flops=1 << 27, bytes_accessed=1 << 20, transcendentals=0),
    )(queries, span_key_value, w_cand, *sources, *partials)


def score_kernel(place_ref, answer_ref, gathered_ref, score_ref, tally_ref):
    parts = gathered_ref.shape[0]
    chains = score_ref.shape[0]
    span = gathered_ref.shape[1] // chains
    logits = functools.reduce(lambda a, b: a + b, [gathered_ref[p] for p in range(parts)])
    top = jnp.max(logits, axis=1, keepdims=True)
    norm = top + jnp.log(jnp.sum(jnp.exp(logits - top), axis=1, keepdims=True))
    lane = lax.broadcasted_iota(jnp.int32, (span, NCAND), 1)
    line = lax.broadcasted_iota(jnp.int32, tally_ref.shape, 0)
    column = lax.broadcasted_iota(jnp.int32, tally_ref.shape, 1)
    tally = jnp.zeros(tally_ref.shape, F32)
    for c in range(chains):
        here = slice(c * span, (c + 1) * span)
        chosen = jnp.sum(jnp.where(lane == answer_ref[c], logits[here], 0.0), axis=1, keepdims=True)
        score = jnp.sum(chosen - norm[here], axis=0, keepdims=True) / span
        score_ref[c : c + 1, :] = jnp.broadcast_to(score, (1, NCAND))
        prompt = (place_ref[2] * chains + c) // SAMPLES
        tally = tally + jnp.where((line == prompt) & (column == answer_ref[c]), score, 0.0)
    tally_ref[...] = tally


def score(gathered, answer_id, place, prompts):
    chains = answer_id.shape[0]
    return pl.pallas_call(
        score_kernel,
        out_shape=(
            jax.ShapeDtypeStruct((chains, NCAND), F32),
            jax.ShapeDtypeStruct((prompts, NCAND), F32),
        ),
        in_specs=[
            pl.BlockSpec(memory_space=pltpu.SMEM),
            pl.BlockSpec(memory_space=pltpu.SMEM),
            pl.BlockSpec(memory_space=VMEM),
        ],
        out_specs=(pl.BlockSpec(memory_space=VMEM),) * 2,
        cost_estimate=pl.CostEstimate(flops=1 << 20, bytes_accessed=1 << 16, transcendentals=0),
    )(place, answer_id, gathered)


def per_device(queries, key_value_cache, slot_tags, span_key_value, answer_id, w_cand):
    owners = lax.axis_size("dp")
    position = lax.axis_index("dp")
    chains_here = queries.shape[0]
    width = key_value_cache.shape[2]
    teams = owners // TEAM
    others = teams - 1
    place = jnp.stack([position % TEAM, position // TEAM, position]).astype(jnp.int32)

    def across(array, step):
        pairs = [(((t + step) % teams) * TEAM + r, t * TEAM + r) for t in range(teams) for r in range(TEAM)]
        return lax.ppermute(array, "dp", pairs)

    def within(array, offset):
        return lax.ppermute(array, "dp", [(i, i ^ offset) for i in range(owners)])

    offsets = range(1, TEAM)
    far = pack([(j, 1, others) for j in offsets], chains_here, owners, place, slot_tags, key_value_cache)
    far_in = [within(m, j) for m, j in zip(far, offsets)]
    visiting = [across(queries, step) for step in range(1, teams)]
    near = pack(
        [(j, 0, 1) for j in offsets] + [(0, 1, others), (0, 0, 1)],
        chains_here, owners, place, slot_tags, key_value_cache,
    )
    near_in = [within(m, j) for m, j in zip(near, offsets)]
    own_far, own_near = near[TEAM - 1], near[TEAM]
    folded = fold(visiting, [own_far] + far_in, width, place)
    partials = [across(m, teams - step) for m, step in zip(folded, range(1, teams))]
    attended, partial_logits = finish(
        queries, span_key_value, w_cand, [own_near] + near_in, partials, width
    )
    gathered = lax.all_gather(partial_logits, "mp")
    prompts = owners * chains_here // SAMPLES
    scores, tally = score(gathered, answer_id, place, prompts)
    chain_score = scores[:, 0]
    step = 1
    while step < owners:
        tally = tally + within(tally, step)
        step *= 2
    per = NCAND // owners
    answer_tally = lax.dynamic_slice_in_dim(tally, position * per, per, axis=1)
    return attended, chain_score, answer_tally


def solution(mesh):
    in_specs = (
        P("dp", None, "mp"),
        P("dp", None, None, "mp"),
        P("dp"),
        P("dp", None, None, "mp"),
        P("dp"),
        P("mp", None),
    )
    out_specs = (P("dp", None, "mp"), P("dp"), P(None, "dp"))
    return jax.shard_map(
        per_device, mesh=mesh, in_specs=in_specs, out_specs=out_specs, check_vma=False
    )
```

```python
import functools

import jax
import jax.numpy as jnp
from jax import lax
from jax.experimental import pallas as pl
from jax.experimental.pallas import tpu as pltpu
from jax.sharding import PartitionSpec as P


QUERY_HEADS = 40
KEY_VALUE_HEADS = 8
HEAD_SIZE = 128
NCAND = 128
PEER = 2
SAMPLES = 16
GROUP = QUERY_HEADS // KEY_VALUE_HEADS
LANES = 128
TEAM = 4
BIG_NEG = -1e30


VMEM = pltpu.VMEM
F32 = jnp.float32
BF16 = jnp.bfloat16


def params(mib=48):
    return pltpu.CompilerParams(vmem_limit_bytes=mib * 1024 * 1024)


def round16(count):
    return (count + 15) // 16 * 16


def note_rows(count):
    return round16(count)


def find_slots(tags_ref, slot_ref, count_ref, chains_here, owners):
    def clear(o, _):
        count_ref[o] = 0
        for k in range(PEER):
            slot_ref[o * PEER + k] = -1
        return 0

    lax.fori_loop(0, owners, clear, 0)

    def place(s, _):
        owner = tags_ref[s] // chains_here
        rank = jnp.minimum(count_ref[owner], PEER - 1)
        slot_ref[owner * PEER + rank] = s
        count_ref[owner] = rank + 1
        return 0

    lax.fori_loop(0, tags_ref.shape[0], place, 0)


def pack_kernel(jobs, chains_here, owners, tags_hbm, cache_ref, *refs):
    outs = refs[: len(jobs)]
    tags_ref, slot_ref, count_ref, tag_sem, sem = refs[len(jobs) :]
    width = cache_ref.shape[2]
    fetch = pltpu.make_async_copy(tags_hbm, tags_ref, tag_sem)
    fetch.start()
    position = lax.axis_index("dp")
    row, high, high_count = lax.rem(position, TEAM), position // TEAM, owners // TEAM
    fetch.wait()
    find_slots(tags_ref, slot_ref, count_ref, chains_here, owners)
    copies = []
    for out, (offset, first, classes) in zip(outs, jobs):
        member = row ^ offset
        blocks = classes * PEER
        note = jnp.full((note_rows(blocks), out.shape[1]), float(chains_here), F32)
        line = lax.broadcasted_iota(jnp.int32, note.shape, 0)
        for h in range(classes):
            owner = lax.rem(high + first + h, high_count) * TEAM + member
            for k in range(PEER):
                slot = slot_ref[owner * PEER + k]
                safe = jnp.maximum(slot, 0)
                chain = jnp.where(slot < 0, chains_here, tags_ref[safe] % chains_here)
                index = h * PEER + k
                for part in range(2):
                    copy = pltpu.make_async_copy(
                        cache_ref.at[safe, part],
                        out.at[pl.ds((index * 2 + part) * width, width)],
                        sem.at[len(copies)],
                    )
                    copy.start()
                    copies.append(copy)
                note = jnp.where(line == index, chain.astype(F32), note)
        out[pl.ds(blocks * 2 * width, note_rows(blocks)), :] = note.astype(BF16)
    for copy in copies:
        copy.wait()


def pack(jobs, chains_here, owners, tags, cache):
    width, lanes = cache.shape[2], cache.shape[3]
    shapes = []
    for _, _, classes in jobs:
        blocks = classes * PEER
        shapes.append(jax.ShapeDtypeStruct((blocks * 2 * width + note_rows(blocks), lanes), BF16))
    moved = sum(s.shape[0] * s.shape[1] * 2 for s in shapes)
    count = sum(classes * PEER * 2 for _, _, classes in jobs)
    return pl.pallas_call(
        functools.partial(pack_kernel, jobs, chains_here, owners),
        out_shape=tuple(shapes),
        in_specs=[pl.BlockSpec(memory_space=pltpu.HBM)] * 2,
        out_specs=tuple(pl.BlockSpec(memory_space=VMEM) for _ in jobs),
        scratch_shapes=[
            pltpu.SMEM(tags.shape, jnp.int32),
            pltpu.SMEM((owners * PEER,), jnp.int32),
            pltpu.SMEM((owners,), jnp.int32),
            pltpu.SemaphoreType.DMA,
            pltpu.SemaphoreType.DMA((count,)),
        ],
        compiler_params=params(51),
        cost_estimate=pl.CostEstimate(flops=0, bytes_accessed=2 * moved, transcendentals=0),
    )(tags, cache)


def query_rows(q_ref, lead, g):
    chains = q_ref.shape[-3]
    tiles = []
    for c in range(chains):
        for j in range(GROUP):
            at = (g * GROUP + j) * HEAD_SIZE
            tiles.append(q_ref[lead + (c, slice(None), pl.ds(at, HEAD_SIZE))])
    return jnp.concatenate(tiles, axis=0)


def dot_nt(a, b):
    return lax.dot_general(a, b, (((1,), (1,)), ((), ())), preferred_element_type=F32)


def block_tiles(sources, h, classes, g, queries, chain_of_row, width):
    scale = HEAD_SIZE**-0.5
    tiles = []
    for source in sources:
        notes = source[pl.ds(classes * PEER * 2 * width, note_rows(classes * PEER)), pl.ds(0, width)].astype(F32)
        for k in range(PEER):
            index = h * PEER + k
            keys = source[pl.ds(index * 2 * width, width), pl.ds(g * HEAD_SIZE, HEAD_SIZE)]
            values = source[pl.ds((index * 2 + 1) * width, width), pl.ds(g * HEAD_SIZE, HEAD_SIZE)]
            valid = notes[index : index + 1, :] == chain_of_row
            scores = jnp.where(valid, dot_nt(queries, keys) * scale, BIG_NEG)
            tiles.append((scores, valid, values))
    return tiles


def reduce_tiles(tiles):
    peak = functools.reduce(jnp.maximum, [jnp.max(s, axis=1, keepdims=True) for s, _, _ in tiles])
    total, summed = None, None
    for scores, valid, values in tiles:
        weights = jnp.where(valid, jnp.exp(scores - peak), 0.0)
        part = jnp.sum(weights, axis=1, keepdims=True)
        added = jnp.dot(weights.astype(BF16), values, preferred_element_type=F32)
        total = part if total is None else total + part
        summed = added if summed is None else summed + added
    return peak, total, summed


def diagonal(rows):
    return lax.broadcasted_iota(jnp.int32, (rows, LANES), 0) == lax.broadcasted_iota(jnp.int32, (rows, LANES), 1)


def pieces_of(rows):
    return [(at, min(LANES, rows - at)) for at in range(0, rows, LANES)]


def fold_kernel(classes, width, *refs):
    q_refs, sources, out_refs = refs[:classes], refs[classes : classes + TEAM], refs[classes + TEAM :]
    chains, span = q_refs[0].shape[0], q_refs[0].shape[1]
    rows = chains * GROUP * span
    heads = q_refs[0].shape[2] // HEAD_SIZE // GROUP
    chain_of_row = (lax.broadcasted_iota(jnp.int32, (rows, width), 0) // (GROUP * span)).astype(F32)
    cuts = pieces_of(rows)
    for h in range(classes):
        out_ref = out_refs[h]
        line = lax.broadcasted_iota(jnp.int32, (out_ref.shape[0] - heads * rows, LANES), 0)
        tail = jnp.zeros(line.shape, F32)
        for g in range(heads):
            queries = query_rows(q_refs[h], (), g)
            peak, total, summed = reduce_tiles(
                block_tiles(sources, h, classes, g, queries, chain_of_row, width)
            )
            empty = total <= 0.0
            safe = jnp.where(empty, 1.0, total)
            out_ref[pl.ds(g * rows, rows), :] = (summed / safe).astype(BF16)
            logs = jnp.where(empty, BIG_NEG, peak + jnp.log(safe))
            for i, (at, size) in enumerate(cuts):
                flat = jnp.sum(
                    jnp.where(diagonal(size), logs[at : at + size, :], 0.0), axis=0, keepdims=True
                )
                first = flat.astype(BF16).astype(F32)
                rest = flat - first
                second = rest.astype(BF16).astype(F32)
                third = rest - second
                for p, piece in enumerate((first, second, third)):
                    at_line = (p * heads + g) * len(cuts) + i
                    tail = jnp.where(line == at_line, piece, tail)
        out_ref[pl.ds(heads * rows, line.shape[0]), :] = tail.astype(BF16)


def message_rows(rows, heads):
    return heads * rows + round16(3 * heads * len(pieces_of(rows)))


def fold(queries, sources, width):
    classes = len(queries)
    chains, span, features = queries[0].shape
    rows, heads = chains * GROUP * span, features // HEAD_SIZE // GROUP
    flops = 4 * classes * heads * rows * TEAM * PEER * width * HEAD_SIZE
    return pl.pallas_call(
        functools.partial(fold_kernel, classes, width),
        out_shape=tuple(
            jax.ShapeDtypeStruct((message_rows(rows, heads), LANES), BF16) for _ in range(classes)
        ),
        in_specs=[pl.BlockSpec(memory_space=VMEM)] * (classes + TEAM),
        out_specs=tuple(pl.BlockSpec(memory_space=VMEM) for _ in range(classes)),
        compiler_params=params(),
        cost_estimate=pl.CostEstimate(flops=flops, bytes_accessed=1 << 20, transcendentals=0),
    )(*queries, *sources)


def finish_kernel(classes, width, *refs):
    q_ref, span_ref, w_ref = refs[:3]
    sources = refs[3 : 3 + TEAM]
    partials = refs[3 + TEAM : 3 + TEAM + classes]
    attended_ref, logits_ref = refs[3 + TEAM + classes :]
    chains, span = q_ref.shape[0], q_ref.shape[1]
    rows = chains * GROUP * span
    heads = q_ref.shape[2] // HEAD_SIZE // GROUP
    scale = HEAD_SIZE**-0.5
    chain_of_row = (lax.broadcasted_iota(jnp.int32, (rows, width), 0) // (GROUP * span)).astype(F32)
    shape = (rows, chains * span)
    row, key = lax.broadcasted_iota(jnp.int32, shape, 0), lax.broadcasted_iota(jnp.int32, shape, 1)
    causal = (row // (GROUP * span) == key // span) & (row % span >= key % span)
    cuts = pieces_of(rows)
    logits = jnp.zeros(logits_ref.shape, F32)
    for g in range(heads):
        queries = query_rows(q_ref, (), g)
        tiles = block_tiles(sources, 0, 1, g, queries, chain_of_row, width)
        lanes = pl.ds(g * HEAD_SIZE, HEAD_SIZE)
        keys = jnp.concatenate([span_ref[c, 0, :, lanes] for c in range(chains)], axis=0)
        values = jnp.concatenate([span_ref[c, 1, :, lanes] for c in range(chains)], axis=0)
        scores = jnp.where(causal, dot_nt(queries, keys) * scale, BIG_NEG)
        tiles.append((scores, causal, values))
        peak, total, summed = reduce_tiles(tiles)
        for partial in partials:
            tail = partial[pl.ds(heads * rows, partial.shape[0] - heads * rows), :].astype(F32)
            columns = []
            for i, (at, size) in enumerate(cuts):
                lines = [(p * heads + g) * len(cuts) + i for p in range(3)]
                flat = sum(tail[n : n + 1, :] for n in lines)
                columns.append(jnp.sum(jnp.where(diagonal(size), flat, 0.0), axis=1, keepdims=True))
            logs = jnp.concatenate(columns, axis=0)
            best = jnp.maximum(peak, logs)
            left, right = jnp.exp(peak - best), jnp.exp(logs - best)
            other = partial[pl.ds(g * rows, rows), :].astype(F32)
            summed = summed * left + other * right
            total = total * left + right
            peak = best
        result = (summed / total).astype(BF16)
        for j in range(GROUP):
            at = (g * GROUP + j) * HEAD_SIZE
            picked = []
            for c in range(chains):
                part = result[(c * GROUP + j) * span : (c * GROUP + j + 1) * span, :]
                attended_ref[c, :, pl.ds(at, HEAD_SIZE)] = part
                picked.append(part)
            logits = logits + jnp.dot(
                jnp.concatenate(picked, axis=0),
                w_ref[pl.ds(at, HEAD_SIZE), :],
                preferred_element_type=F32,
            )
    logits_ref[...] = logits


def finish(queries, span_key_value, w_cand, sources, partials, width):
    chains, span, _ = queries.shape
    return pl.pallas_call(
        functools.partial(finish_kernel, len(partials), width),
        out_shape=(
            jax.ShapeDtypeStruct(queries.shape, BF16),
            jax.ShapeDtypeStruct((chains * span, NCAND), F32),
        ),
        in_specs=[pl.BlockSpec(memory_space=VMEM)] * (3 + TEAM + len(partials)),
        out_specs=(pl.BlockSpec(memory_space=VMEM),) * 2,
        compiler_params=params(),
        cost_estimate=pl.CostEstimate(flops=1 << 27, bytes_accessed=1 << 20, transcendentals=0),
    )(queries, span_key_value, w_cand, *sources, *partials)


def score_kernel(answer_ref, gathered_ref, score_ref, tally_ref):
    parts = gathered_ref.shape[0]
    position = lax.axis_index("dp")
    chains = score_ref.shape[0]
    span = gathered_ref.shape[1] // chains
    logits = functools.reduce(lambda a, b: a + b, [gathered_ref[p] for p in range(parts)])
    top = jnp.max(logits, axis=1, keepdims=True)
    norm = top + jnp.log(jnp.sum(jnp.exp(logits - top), axis=1, keepdims=True))
    lane = lax.broadcasted_iota(jnp.int32, (span, NCAND), 1)
    line = lax.broadcasted_iota(jnp.int32, tally_ref.shape, 0)
    column = lax.broadcasted_iota(jnp.int32, tally_ref.shape, 1)
    tally = jnp.zeros(tally_ref.shape, F32)
    for c in range(chains):
        here = slice(c * span, (c + 1) * span)
        chosen = jnp.sum(jnp.where(lane == answer_ref[c], logits[here], 0.0), axis=1, keepdims=True)
        score = jnp.sum(chosen - norm[here], axis=0, keepdims=True) / span
        score_ref[c : c + 1, :] = jnp.broadcast_to(score, (1, NCAND))
        prompt = (position * chains + c) // SAMPLES
        tally = tally + jnp.where((line == prompt) & (column == answer_ref[c]), score, 0.0)
    tally_ref[...] = tally


def score(gathered, answer_id, prompts):
    chains = answer_id.shape[0]
    return pl.pallas_call(
        score_kernel,
        out_shape=(
            jax.ShapeDtypeStruct((chains, NCAND), F32),
            jax.ShapeDtypeStruct((prompts, NCAND), F32),
        ),
        in_specs=[pl.BlockSpec(memory_space=pltpu.SMEM), pl.BlockSpec(memory_space=VMEM)],
        out_specs=(pl.BlockSpec(memory_space=VMEM),) * 2,
        compiler_params=params(8),
        cost_estimate=pl.CostEstimate(flops=1 << 20, bytes_accessed=1 << 16, transcendentals=0),
    )(answer_id, gathered)


def program(queries, key_value_cache, slot_tags, span_key_value, answer_id, w_cand):
    owners = lax.axis_size("dp")
    chains_here = queries.shape[0]
    width = key_value_cache.shape[2]
    teams = owners // TEAM
    others = teams - 1

    def across(array, step):
        pairs = [(((t + step) % teams) * TEAM + r, t * TEAM + r) for t in range(teams) for r in range(TEAM)]
        return lax.ppermute(array, "dp", pairs)

    def within(array, offset):
        return lax.ppermute(array, "dp", [(i, i ^ offset) for i in range(owners)])

    offsets = range(1, TEAM)
    jobs = [(j, 1, others) for j in offsets] + [(j, 0, 1) for j in offsets] + [(0, 1, others), (0, 0, 1)]
    messages = pack(jobs, chains_here, owners, slot_tags, key_value_cache)
    far_in = [within(m, j) for m, j in zip(messages, offsets)]
    visiting = [across(queries, step) for step in range(1, teams)]
    near_in = [within(m, j) for m, j in zip(messages[TEAM - 1 :], offsets)]
    own_far, own_near = messages[-2:]
    folded = fold(visiting, [own_far] + far_in, width)
    partials = [across(m, teams - step) for m, step in zip(folded, range(1, teams))]
    attended, partial_logits = finish(
        queries, span_key_value, w_cand, [own_near] + near_in, partials, width
    )
    gathered = lax.all_gather(partial_logits, "mp")
    prompts = owners * chains_here // SAMPLES
    scores, tally = score(gathered, answer_id, prompts)
    chain_score = scores[:, 0]
    step = 1
    while step < owners:
        tally = tally + within(tally, step)
        step *= 2
    per = NCAND // owners
    answer_tally = lax.dynamic_slice_in_dim(tally, lax.axis_index("dp") * per, per, axis=1)
    return attended, chain_score, answer_tally


def solution(mesh):
    in_specs = (
        P("dp", None, "mp"),
        P("dp", None, None, "mp"),
        P("dp"),
        P("dp", None, None, "mp"),
        P("dp"),
        P("mp", None),
    )
    out_specs = (P("dp", None, "mp"), P("dp"), P(None, "dp"))
    return jax.shard_map(program, mesh=mesh, in_specs=in_specs, out_specs=out_specs, check_vma=False)
```

```python
import functools

import jax
import jax.numpy as jnp
from jax import lax
from jax.experimental import pallas as pl
from jax.experimental.pallas import tpu as pltpu
from jax.sharding import PartitionSpec as P


QUERY_HEADS = 40
KEY_VALUE_HEADS = 8
HEAD_SIZE = 128
NCAND = 128
PEER = 2
SAMPLES = 16
GROUP = QUERY_HEADS // KEY_VALUE_HEADS
LANES = 128
TEAM = 4
DIAGONAL = 3
BIG_NEG = -1e30


VMEM = pltpu.VMEM
F32 = jnp.float32
BF16 = jnp.bfloat16


def params(mib=48):
    return pltpu.CompilerParams(vmem_limit_bytes=mib * 1024 * 1024)


def round16(count):
    return (count + 15) // 16 * 16


def note_rows(count):
    return (count + 7) // 8 * 8


def find_slots(tags_ref, slot_ref, count_ref, chains_here, owners):
    def clear(o, _):
        count_ref[o] = 0
        for k in range(PEER):
            slot_ref[o * PEER + k] = -1
        return 0

    lax.fori_loop(0, owners, clear, 0)

    def place(s, _):
        owner = tags_ref[s] // chains_here
        rank = jnp.minimum(count_ref[owner], PEER - 1)
        slot_ref[owner * PEER + rank] = s
        count_ref[owner] = rank + 1
        return 0

    lax.fori_loop(0, tags_ref.shape[0], place, 0)


def pack_kernel(jobs, chains_here, owners, tags_hbm, cache_ref, *refs):
    outs = refs[: len(jobs)]
    tags_ref, slot_ref, count_ref, tag_sem, sem = refs[len(jobs) :]
    width = cache_ref.shape[2]
    fetch = pltpu.make_async_copy(tags_hbm, tags_ref, tag_sem)
    fetch.start()
    position = lax.axis_index("dp")
    row, high, high_count = lax.rem(position, TEAM), position // TEAM, owners // TEAM
    fetch.wait()
    find_slots(tags_ref, slot_ref, count_ref, chains_here, owners)
    copies = []
    for out, (offset, first, classes) in zip(outs, jobs):
        member = row ^ offset
        blocks = classes * PEER
        note = jnp.full((note_rows(blocks), out.shape[1]), float(chains_here), F32)
        line = lax.broadcasted_iota(jnp.int32, note.shape, 0)
        for h in range(classes):
            owner = lax.rem(high + first + h, high_count) * TEAM + member
            for k in range(PEER):
                slot = slot_ref[owner * PEER + k]
                safe = jnp.maximum(slot, 0)
                chain = jnp.where(slot < 0, chains_here, tags_ref[safe] % chains_here)
                index = h * PEER + k
                for part in range(2):
                    copy = pltpu.make_async_copy(
                        cache_ref.at[safe, part],
                        out.at[pl.ds((index * 2 + part) * width, width)],
                        sem.at[len(copies)],
                    )
                    copy.start()
                    copies.append(copy)
                note = jnp.where(line == index, chain.astype(F32), note)
        out[pl.ds(blocks * 2 * width, note_rows(blocks)), :] = note.astype(BF16)
    for copy in copies:
        copy.wait()


def pack(jobs, chains_here, owners, tags, cache):
    width, lanes = cache.shape[2], cache.shape[3]
    shapes = []
    for _, _, classes in jobs:
        blocks = classes * PEER
        shapes.append(jax.ShapeDtypeStruct((blocks * 2 * width + note_rows(blocks), lanes), BF16))
    moved = sum(s.shape[0] * s.shape[1] * 2 for s in shapes)
    count = sum(classes * PEER * 2 for _, _, classes in jobs)
    return pl.pallas_call(
        functools.partial(pack_kernel, jobs, chains_here, owners),
        out_shape=tuple(shapes),
        in_specs=[pl.BlockSpec(memory_space=pltpu.HBM)] * 2,
        out_specs=tuple(pl.BlockSpec(memory_space=VMEM) for _ in jobs),
        scratch_shapes=[
            pltpu.SMEM(tags.shape, jnp.int32),
            pltpu.SMEM((owners * PEER,), jnp.int32),
            pltpu.SMEM((owners,), jnp.int32),
            pltpu.SemaphoreType.DMA,
            pltpu.SemaphoreType.DMA((count,)),
        ],
        compiler_params=params(),
        cost_estimate=pl.CostEstimate(flops=0, bytes_accessed=2 * moved, transcendentals=0),
    )(tags, cache)


def query_rows(q_ref, lead, g):
    chains = q_ref.shape[-3]
    tiles = []
    for c in range(chains):
        for j in range(GROUP):
            at = (g * GROUP + j) * HEAD_SIZE
            tiles.append(q_ref[lead + (c, slice(None), pl.ds(at, HEAD_SIZE))])
    return jnp.concatenate(tiles, axis=0)


def dot_nt(a, b):
    return lax.dot_general(a, b, (((1,), (1,)), ((), ())), preferred_element_type=F32)


def block_tiles(sources, h, classes, g, queries, chain_of_row, width):
    scale = HEAD_SIZE**-0.5
    tiles = []
    for source in sources:
        notes = source[pl.ds(classes * PEER * 2 * width, note_rows(classes * PEER)), pl.ds(0, width)].astype(F32)
        for k in range(PEER):
            index = h * PEER + k
            keys = source[pl.ds(index * 2 * width, width), pl.ds(g * HEAD_SIZE, HEAD_SIZE)]
            values = source[pl.ds((index * 2 + 1) * width, width), pl.ds(g * HEAD_SIZE, HEAD_SIZE)]
            valid = notes[index : index + 1, :] == chain_of_row
            scores = jnp.where(valid, dot_nt(queries, keys) * scale, BIG_NEG)
            tiles.append((scores, valid, values))
    return tiles


def reduce_tiles(tiles):
    peak = functools.reduce(jnp.maximum, [jnp.max(s, axis=1, keepdims=True) for s, _, _ in tiles])
    total, summed = None, None
    for scores, valid, values in tiles:
        weights = jnp.where(valid, jnp.exp(scores - peak), 0.0)
        part = jnp.sum(weights, axis=1, keepdims=True)
        added = jnp.dot(weights.astype(BF16), values, preferred_element_type=F32)
        total = part if total is None else total + part
        summed = added if summed is None else summed + added
    return peak, total, summed


def diagonal(rows):
    return lax.broadcasted_iota(jnp.int32, (rows, LANES), 0) == lax.broadcasted_iota(jnp.int32, (rows, LANES), 1)


def pieces_of(rows):
    return [(at, min(LANES, rows - at)) for at in range(0, rows, LANES)]


def fold_kernel(classes, held, width, *refs):
    q_refs, sources, out_refs = refs[:classes], refs[classes : classes + held], refs[classes + held :]
    chains, span = q_refs[0].shape[0], q_refs[0].shape[1]
    rows = chains * GROUP * span
    heads = q_refs[0].shape[2] // HEAD_SIZE // GROUP
    chain_of_row = (lax.broadcasted_iota(jnp.int32, (rows, width), 0) // (GROUP * span)).astype(F32)
    cuts = pieces_of(rows)
    for h in range(classes):
        out_ref = out_refs[h]
        line = lax.broadcasted_iota(jnp.int32, (out_ref.shape[0] - heads * rows, LANES), 0)
        tail = jnp.zeros(line.shape, F32)
        for g in range(heads):
            queries = query_rows(q_refs[h], (), g)
            peak, total, summed = reduce_tiles(
                block_tiles(sources, h, classes, g, queries, chain_of_row, width)
            )
            empty = total <= 0.0
            safe = jnp.where(empty, 1.0, total)
            out_ref[pl.ds(g * rows, rows), :] = (summed / safe).astype(BF16)
            logs = jnp.where(empty, BIG_NEG, peak + jnp.log(safe))
            for i, (at, size) in enumerate(cuts):
                flat = jnp.sum(
                    jnp.where(diagonal(size), logs[at : at + size, :], 0.0), axis=0, keepdims=True
                )
                first = flat.astype(BF16).astype(F32)
                rest = flat - first
                second = rest.astype(BF16).astype(F32)
                third = rest - second
                for p, piece in enumerate((first, second, third)):
                    at_line = (p * heads + g) * len(cuts) + i
                    tail = jnp.where(line == at_line, piece, tail)
        out_ref[pl.ds(heads * rows, line.shape[0]), :] = tail.astype(BF16)


def message_rows(rows, heads):
    return heads * rows + round16(3 * heads * len(pieces_of(rows)))


def fold(queries, sources, width):
    classes = len(queries)
    chains, span, features = queries[0].shape
    rows, heads = chains * GROUP * span, features // HEAD_SIZE // GROUP
    held = len(sources)
    flops = 4 * classes * heads * rows * held * PEER * width * HEAD_SIZE
    return pl.pallas_call(
        functools.partial(fold_kernel, classes, held, width),
        out_shape=tuple(
            jax.ShapeDtypeStruct((message_rows(rows, heads), LANES), BF16) for _ in range(classes)
        ),
        in_specs=[pl.BlockSpec(memory_space=VMEM)] * (classes + held),
        out_specs=tuple(pl.BlockSpec(memory_space=VMEM) for _ in range(classes)),
        compiler_params=params(),
        cost_estimate=pl.CostEstimate(flops=flops, bytes_accessed=1 << 20, transcendentals=0),
    )(*queries, *sources)


def own_kernel(width, *refs):
    q_ref, span_ref = refs[:2]
    sources, (rows_ref, logs_ref) = refs[2:-2], refs[-2:]
    chains, span = q_ref.shape[0], q_ref.shape[1]
    rows = chains * GROUP * span
    heads = q_ref.shape[2] // HEAD_SIZE // GROUP
    scale = HEAD_SIZE**-0.5
    chain_of_row = (lax.broadcasted_iota(jnp.int32, (rows, width), 0) // (GROUP * span)).astype(F32)
    shape = (rows, chains * span)
    row, key = lax.broadcasted_iota(jnp.int32, shape, 0), lax.broadcasted_iota(jnp.int32, shape, 1)
    causal = (row // (GROUP * span) == key // span) & (row % span >= key % span)
    for g in range(heads):
        queries = query_rows(q_ref, (), g)
        tiles = block_tiles(sources, 0, 1, g, queries, chain_of_row, width)
        lanes = pl.ds(g * HEAD_SIZE, HEAD_SIZE)
        keys = jnp.concatenate([span_ref[c, 0, :, lanes] for c in range(chains)], axis=0)
        values = jnp.concatenate([span_ref[c, 1, :, lanes] for c in range(chains)], axis=0)
        scores = jnp.where(causal, dot_nt(queries, keys) * scale, BIG_NEG)
        tiles.append((scores, causal, values))
        peak, total, summed = reduce_tiles(tiles)
        rows_ref[pl.ds(g * rows, rows), :] = summed / total
        logs_ref[pl.ds(g * rows, rows), :] = jnp.broadcast_to(peak + jnp.log(total), (rows, LANES))


def own(queries, span_key_value, sources, width):
    chains, span, features = queries.shape
    rows, heads = chains * GROUP * span, features // HEAD_SIZE // GROUP
    flops = 4 * heads * rows * len(sources) * PEER * width * HEAD_SIZE
    return pl.pallas_call(
        functools.partial(own_kernel, width),
        out_shape=(jax.ShapeDtypeStruct((heads * rows, LANES), F32),) * 2,
        in_specs=[pl.BlockSpec(memory_space=VMEM)] * (2 + len(sources)),
        out_specs=(pl.BlockSpec(memory_space=VMEM),) * 2,
        compiler_params=params(),
        cost_estimate=pl.CostEstimate(flops=flops, bytes_accessed=1 << 20, transcendentals=0),
    )(queries, span_key_value, *sources)


def finish_kernel(chains, span, *refs):
    rows_ref, logs_ref, w_ref = refs[:3]
    partials, (attended_ref, logits_ref) = refs[3:-2], refs[-2:]
    rows = chains * GROUP * span
    heads = rows_ref.shape[0] // rows
    cuts = pieces_of(rows)
    logits = jnp.zeros(logits_ref.shape, F32)
    for g in range(heads):
        here = pl.ds(g * rows, rows)
        items = [(rows_ref[here, :], logs_ref[here, :])]
        for partial in partials:
            tail = partial[pl.ds(heads * rows, partial.shape[0] - heads * rows), :].astype(F32)
            columns = []
            for i, (at, size) in enumerate(cuts):
                lines = [(p * heads + g) * len(cuts) + i for p in range(3)]
                flat = sum(tail[n : n + 1, :] for n in lines)
                columns.append(jnp.sum(jnp.where(diagonal(size), flat, 0.0), axis=1, keepdims=True))
            logs = jnp.concatenate(columns, axis=0)
            items.append((partial[here, :].astype(F32), logs))
        best = functools.reduce(jnp.maximum, [logs for _, logs in items])
        shares = [jnp.exp(logs - best) for _, logs in items]
        total = functools.reduce(jnp.add, shares)
        summed = functools.reduce(jnp.add, [x * w for (x, _), w in zip(items, shares)])
        result = (summed / total).astype(BF16)
        for j in range(GROUP):
            at = (g * GROUP + j) * HEAD_SIZE
            picked = []
            for c in range(chains):
                part = result[(c * GROUP + j) * span : (c * GROUP + j + 1) * span, :]
                attended_ref[c, :, pl.ds(at, HEAD_SIZE)] = part
                picked.append(part)
            logits = logits + jnp.dot(
                jnp.concatenate(picked, axis=0),
                w_ref[pl.ds(at, HEAD_SIZE), :],
                preferred_element_type=F32,
            )
    logits_ref[...] = logits


def finish(shape, mine, w_cand, partials):
    chains, span, _ = shape
    return pl.pallas_call(
        functools.partial(finish_kernel, chains, span),
        out_shape=(
            jax.ShapeDtypeStruct(shape, BF16),
            jax.ShapeDtypeStruct((chains * span, NCAND), F32),
        ),
        in_specs=[pl.BlockSpec(memory_space=VMEM)] * (3 + len(partials)),
        out_specs=(pl.BlockSpec(memory_space=VMEM),) * 2,
        compiler_params=params(),
        cost_estimate=pl.CostEstimate(flops=1 << 24, bytes_accessed=1 << 20, transcendentals=0),
    )(*mine, w_cand, *partials)


def score_kernel(answer_ref, gathered_ref, score_ref, tally_ref):
    parts = gathered_ref.shape[0]
    position = lax.axis_index("dp")
    chains = score_ref.shape[0]
    span = gathered_ref.shape[1] // chains
    logits = functools.reduce(lambda a, b: a + b, [gathered_ref[p] for p in range(parts)])
    top = jnp.max(logits, axis=1, keepdims=True)
    norm = top + jnp.log(jnp.sum(jnp.exp(logits - top), axis=1, keepdims=True))
    lane = lax.broadcasted_iota(jnp.int32, (span, NCAND), 1)
    line = lax.broadcasted_iota(jnp.int32, tally_ref.shape, 0)
    column = lax.broadcasted_iota(jnp.int32, tally_ref.shape, 1)
    tally = jnp.zeros(tally_ref.shape, F32)
    for c in range(chains):
        here = slice(c * span, (c + 1) * span)
        chosen = jnp.sum(jnp.where(lane == answer_ref[c], logits[here], 0.0), axis=1, keepdims=True)
        score = jnp.sum(chosen - norm[here], axis=0, keepdims=True) / span
        score_ref[c : c + 1, :] = jnp.broadcast_to(score, (1, NCAND))
        prompt = (position * chains + c) // SAMPLES
        tally = tally + jnp.where((line == prompt) & (column == answer_ref[c]), score, 0.0)
    tally_ref[...] = tally


def score(gathered, answer_id, prompts):
    chains = answer_id.shape[0]
    return pl.pallas_call(
        score_kernel,
        out_shape=(
            jax.ShapeDtypeStruct((chains, NCAND), F32),
            jax.ShapeDtypeStruct((prompts, NCAND), F32),
        ),
        in_specs=[pl.BlockSpec(memory_space=pltpu.SMEM), pl.BlockSpec(memory_space=VMEM)],
        out_specs=(pl.BlockSpec(memory_space=VMEM),) * 2,
        compiler_params=params(8),
        cost_estimate=pl.CostEstimate(flops=1 << 20, bytes_accessed=1 << 16, transcendentals=0),
    )(answer_id, gathered)


def program(queries, key_value_cache, slot_tags, span_key_value, answer_id, w_cand):
    owners = lax.axis_size("dp")
    chains_here = queries.shape[0]
    width = key_value_cache.shape[2]
    teams = owners // TEAM
    others = teams - 1

    def across(array, step):
        pairs = [(((t + step) % teams) * TEAM + r, t * TEAM + r) for t in range(teams) for r in range(TEAM)]
        return lax.ppermute(array, "dp", pairs)

    def within(array, offset):
        return lax.ppermute(array, "dp", [(i, i ^ offset) for i in range(owners)])

    offsets = range(1, TEAM)
    slot_tags = pltpu.with_memory_space_constraint(slot_tags, pltpu.HBM)
    key_value_cache = pltpu.with_memory_space_constraint(key_value_cache, pltpu.HBM)
    sort = functools.partial(pack, chains_here=chains_here, owners=owners, tags=slot_tags, cache=key_value_cache)
    messages = sort([(j, 1, others) for j in offsets])
    far_in = [within(m, j) for m, j in zip(messages, offsets)]
    visiting = [across(queries, step) for step in range(1, teams)]
    mate = within(queries, DIAGONAL)
    near = sort([(1, 0, 1), (2, 0, 1), (DIAGONAL, 0, 1), (0, 1, others), (0, 0, 1)])
    near_in = [within(near[0], 1), within(near[1], 2)]
    folded = fold(visiting, [near[3]] + far_in, width)
    partials = [across(m, teams - step) for m, step in zip(folded, range(1, teams))]
    answer = fold([mate], [near[2]], width)
    partials = [within(answer[0], DIAGONAL)] + partials
    mine = own(queries, span_key_value, [near[4]] + near_in, width)
    attended, partial_logits = finish(queries.shape, mine, w_cand, partials)
    gathered = lax.all_gather(partial_logits, "mp")
    prompts = owners * chains_here // SAMPLES
    scores, tally = score(gathered, answer_id, prompts)
    chain_score = scores[:, 0]
    step = 1
    while step < owners:
        tally = tally + within(tally, step)
        step *= 2
    per = NCAND // owners
    answer_tally = lax.dynamic_slice_in_dim(tally, lax.axis_index("dp") * per, per, axis=1)
    return attended, chain_score, answer_tally


def solution(mesh):
    in_specs = (
        P("dp", None, "mp"),
        P("dp", None, None, "mp"),
        P("dp"),
        P("dp", None, None, "mp"),
        P("dp"),
        P("mp", None),
    )
    out_specs = (P("dp", None, "mp"), P("dp"), P(None, "dp"))
    return jax.shard_map(program, mesh=mesh, in_specs=in_specs, out_specs=out_specs, check_vma=False)
```

```python
import functools

import jax
import jax.numpy as jnp
from jax import lax
from jax.experimental import pallas as pl
from jax.experimental.pallas import tpu as pltpu
from jax.sharding import PartitionSpec as P


QUERY_HEADS = 40
KEY_VALUE_HEADS = 8
HEAD_SIZE = 128
NCAND = 128
PEER = 2
SAMPLES = 16
GROUP = QUERY_HEADS // KEY_VALUE_HEADS
LANES = 128
TEAM = 4
DIAGONAL = 3
PULLS = 4
BIG_NEG = -1e30


VMEM = pltpu.VMEM
F32 = jnp.float32
BF16 = jnp.bfloat16


def params(mib=48):
    return pltpu.CompilerParams(vmem_limit_bytes=mib * 1024 * 1024)


def round16(count):
    return (count + 15) // 16 * 16


def note_rows(count):
    return (count + 7) // 8 * 8


def find_slots(tags_ref, slot_ref, count_ref, chains_here, owners):
    for o in range(owners):
        count_ref[o] = 0
        for k in range(PEER):
            slot_ref[o * PEER + k] = -1
    for s in range(tags_ref.shape[0]):
        owner = lax.div(tags_ref[s], chains_here)
        rank = jnp.minimum(count_ref[owner], PEER - 1)
        slot_ref[owner * PEER + rank] = s
        count_ref[owner] = rank + 1


def pack_kernel(jobs, chains_here, owners, tags_hbm, cache_hbm, *refs):
    outs = refs[: len(jobs)]
    cache_ref, tags_ref, slot_ref, count_ref, tag_sem, sem = refs[len(jobs) :]
    fetch = pltpu.make_async_copy(tags_hbm, tags_ref, tag_sem)
    fetch.start()
    slots, length = cache_ref.shape[:2]
    step = -(-slots // sem.shape[0])
    pulls = []
    for i, at in enumerate(range(0, slots, step)):
        here = pl.ds(at, min(step, slots - at))
        pulls.append(pltpu.make_async_copy(cache_hbm.at[here], cache_ref.at[here], sem.at[i]))
        pulls[-1].start()
    position = lax.axis_index("dp")
    row, high, high_count = lax.rem(position, TEAM), lax.div(position, TEAM), owners // TEAM
    fetch.wait()
    find_slots(tags_ref, slot_ref, count_ref, chains_here, owners)
    picks = []
    for out, (offset, first, classes) in zip(outs, jobs):
        member = row ^ offset
        blocks = classes * PEER
        note = jnp.full((note_rows(blocks), out.shape[1]), float(chains_here), F32)
        line = lax.broadcasted_iota(jnp.int32, note.shape, 0)
        for h in range(classes):
            owner = lax.rem(high + first + h, high_count) * TEAM + member
            for k in range(PEER):
                slot = slot_ref[owner * PEER + k]
                safe = jnp.maximum(slot, 0)
                chain = jnp.where(slot < 0, chains_here, lax.rem(tags_ref[safe], chains_here))
                index = h * PEER + k
                note = jnp.where(line == index, chain.astype(F32), note)
                picks.append((out, index, safe))
        out[pl.ds(blocks * length, note_rows(blocks)), :] = note.astype(BF16)
    for pull in pulls:
        pull.wait()
    for out, index, safe in picks:
        out[pl.ds(index * length, length), :] = cache_ref[safe]


def pack(jobs, chains_here, owners, tags, cache):
    _, length, lanes = cache.shape
    shapes = []
    for _, _, classes in jobs:
        blocks = classes * PEER
        shapes.append(jax.ShapeDtypeStruct((blocks * length + note_rows(blocks), lanes), BF16))
    return pl.pallas_call(
        functools.partial(pack_kernel, jobs, chains_here, owners),
        out_shape=tuple(shapes),
        in_specs=[pl.BlockSpec(memory_space=pltpu.HBM)] * 2,
        out_specs=tuple(pl.BlockSpec(memory_space=VMEM) for _ in jobs),
        scratch_shapes=[
            VMEM(cache.shape, BF16),
            pltpu.SMEM(tags.shape, jnp.int32),
            pltpu.SMEM((owners * PEER,), jnp.int32),
            pltpu.SMEM((owners,), jnp.int32),
            pltpu.SemaphoreType.DMA,
            pltpu.SemaphoreType.DMA((PULLS,)),
        ],
        compiler_params=params(),
        cost_estimate=pl.CostEstimate(flops=0, bytes_accessed=cache.size * 2, transcendentals=0),
    )(tags, cache)


def query_rows(q_ref, lead, g):
    chains = q_ref.shape[-3]
    tiles = []
    for c in range(chains):
        for j in range(GROUP):
            at = (g * GROUP + j) * HEAD_SIZE
            tiles.append(q_ref[lead + (c, slice(None), pl.ds(at, HEAD_SIZE))])
    return jnp.concatenate(tiles, axis=0)


def dot_nt(a, b):
    return lax.dot_general(a, b, (((1,), (1,)), ((), ())), preferred_element_type=F32)


def block_tiles(sources, h, classes, g, queries, chain_of_row, width):
    scale = HEAD_SIZE**-0.5
    tiles = []
    for source in sources:
        notes = source[pl.ds(classes * PEER * 2 * width, note_rows(classes * PEER)), pl.ds(0, width)].astype(F32)
        for k in range(PEER):
            index = h * PEER + k
            keys = source[pl.ds(index * 2 * width, width), pl.ds(g * HEAD_SIZE, HEAD_SIZE)]
            values = source[pl.ds((index * 2 + 1) * width, width), pl.ds(g * HEAD_SIZE, HEAD_SIZE)]
            valid = notes[index : index + 1, :] == chain_of_row
            scores = jnp.where(valid, dot_nt(queries, keys) * scale, BIG_NEG)
            tiles.append((scores, valid, values))
    return tiles


def reduce_tiles(tiles):
    peak = functools.reduce(jnp.maximum, [jnp.max(s, axis=1, keepdims=True) for s, _, _ in tiles])
    total, summed = None, None
    for scores, valid, values in tiles:
        weights = jnp.where(valid, jnp.exp(scores - peak), 0.0)
        part = jnp.sum(weights, axis=1, keepdims=True)
        added = jnp.dot(weights.astype(BF16), values, preferred_element_type=F32)
        total = part if total is None else total + part
        summed = added if summed is None else summed + added
    return peak, total, summed


def diagonal(rows):
    return lax.broadcasted_iota(jnp.int32, (rows, LANES), 0) == lax.broadcasted_iota(jnp.int32, (rows, LANES), 1)


def pieces_of(rows):
    return [(at, min(LANES, rows - at)) for at in range(0, rows, LANES)]


def fold_kernel(classes, held, width, *refs):
    q_refs, sources, out_refs = refs[:classes], refs[classes : classes + held], refs[classes + held :]
    chains, span = q_refs[0].shape[0], q_refs[0].shape[1]
    rows = chains * GROUP * span
    heads = q_refs[0].shape[2] // HEAD_SIZE // GROUP
    chain_of_row = (lax.broadcasted_iota(jnp.int32, (rows, width), 0) // (GROUP * span)).astype(F32)
    cuts = pieces_of(rows)
    for h in range(classes):
        out_ref = out_refs[h]
        line = lax.broadcasted_iota(jnp.int32, (out_ref.shape[0] - heads * rows, LANES), 0)
        tail = jnp.zeros(line.shape, F32)
        for g in range(heads):
            queries = query_rows(q_refs[h], (), g)
            peak, total, summed = reduce_tiles(
                block_tiles(sources, h, classes, g, queries, chain_of_row, width)
            )
            empty = total <= 0.0
            safe = jnp.where(empty, 1.0, total)
            out_ref[pl.ds(g * rows, rows), :] = (summed / safe).astype(BF16)
            logs = jnp.where(empty, BIG_NEG, peak + jnp.log(safe))
            for i, (at, size) in enumerate(cuts):
                flat = jnp.sum(
                    jnp.where(diagonal(size), logs[at : at + size, :], 0.0), axis=0, keepdims=True
                )
                first = flat.astype(BF16).astype(F32)
                rest = flat - first
                second = rest.astype(BF16).astype(F32)
                third = rest - second
                for p, piece in enumerate((first, second, third)):
                    at_line = (p * heads + g) * len(cuts) + i
                    tail = jnp.where(line == at_line, piece, tail)
        out_ref[pl.ds(heads * rows, line.shape[0]), :] = tail.astype(BF16)


def message_rows(rows, heads):
    return heads * rows + round16(3 * heads * len(pieces_of(rows)))


def fold(queries, sources, width):
    classes = len(queries)
    chains, span, features = queries[0].shape
    rows, heads = chains * GROUP * span, features // HEAD_SIZE // GROUP
    held = len(sources)
    flops = 4 * classes * heads * rows * held * PEER * width * HEAD_SIZE
    return pl.pallas_call(
        functools.partial(fold_kernel, classes, held, width),
        out_shape=tuple(
            jax.ShapeDtypeStruct((message_rows(rows, heads), LANES), BF16) for _ in range(classes)
        ),
        in_specs=[pl.BlockSpec(memory_space=VMEM)] * (classes + held),
        out_specs=tuple(pl.BlockSpec(memory_space=VMEM) for _ in range(classes)),
        compiler_params=params(),
        cost_estimate=pl.CostEstimate(flops=flops, bytes_accessed=1 << 20, transcendentals=0),
    )(*queries, *sources)


def own_kernel(width, *refs):
    q_ref, span_ref = refs[:2]
    sources, (rows_ref, logs_ref) = refs[2:-2], refs[-2:]
    chains, span = q_ref.shape[0], q_ref.shape[1]
    rows = chains * GROUP * span
    heads = q_ref.shape[2] // HEAD_SIZE // GROUP
    scale = HEAD_SIZE**-0.5
    chain_of_row = (lax.broadcasted_iota(jnp.int32, (rows, width), 0) // (GROUP * span)).astype(F32)
    shape = (rows, chains * span)
    row, key = lax.broadcasted_iota(jnp.int32, shape, 0), lax.broadcasted_iota(jnp.int32, shape, 1)
    causal = (row // (GROUP * span) == key // span) & (row % span >= key % span)
    for g in range(heads):
        queries = query_rows(q_ref, (), g)
        tiles = block_tiles(sources, 0, 1, g, queries, chain_of_row, width)
        lanes = pl.ds(g * HEAD_SIZE, HEAD_SIZE)
        keys = jnp.concatenate([span_ref[c, 0, :, lanes] for c in range(chains)], axis=0)
        values = jnp.concatenate([span_ref[c, 1, :, lanes] for c in range(chains)], axis=0)
        scores = jnp.where(causal, dot_nt(queries, keys) * scale, BIG_NEG)
        tiles.append((scores, causal, values))
        peak, total, summed = reduce_tiles(tiles)
        rows_ref[pl.ds(g * rows, rows), :] = summed / total
        logs_ref[pl.ds(g * rows, rows), :] = jnp.broadcast_to(peak + jnp.log(total), (rows, LANES))


def own(queries, span_key_value, sources, width):
    chains, span, features = queries.shape
    rows, heads = chains * GROUP * span, features // HEAD_SIZE // GROUP
    flops = 4 * heads * rows * len(sources) * PEER * width * HEAD_SIZE
    return pl.pallas_call(
        functools.partial(own_kernel, width),
        out_shape=(jax.ShapeDtypeStruct((heads * rows, LANES), F32),) * 2,
        in_specs=[pl.BlockSpec(memory_space=VMEM)] * (2 + len(sources)),
        out_specs=(pl.BlockSpec(memory_space=VMEM),) * 2,
        compiler_params=params(),
        cost_estimate=pl.CostEstimate(flops=flops, bytes_accessed=1 << 20, transcendentals=0),
    )(queries, span_key_value, *sources)


def finish_kernel(chains, span, *refs):
    rows_ref, logs_ref, w_ref = refs[:3]
    partials, (attended_ref, logits_ref) = refs[3:-2], refs[-2:]
    rows = chains * GROUP * span
    heads = rows_ref.shape[0] // rows
    cuts = pieces_of(rows)
    logits = jnp.zeros(logits_ref.shape, F32)
    for g in range(heads):
        here = pl.ds(g * rows, rows)
        items = [(rows_ref[here, :], logs_ref[here, :])]
        for partial in partials:
            tail = partial[pl.ds(heads * rows, partial.shape[0] - heads * rows), :].astype(F32)
            columns = []
            for i, (at, size) in enumerate(cuts):
                lines = [(p * heads + g) * len(cuts) + i for p in range(3)]
                flat = sum(tail[n : n + 1, :] for n in lines)
                columns.append(jnp.sum(jnp.where(diagonal(size), flat, 0.0), axis=1, keepdims=True))
            logs = jnp.concatenate(columns, axis=0)
            items.append((partial[here, :].astype(F32), logs))
        best = functools.reduce(jnp.maximum, [logs for _, logs in items])
        shares = [jnp.exp(logs - best) for _, logs in items]
        total = functools.reduce(jnp.add, shares)
        summed = functools.reduce(jnp.add, [x * w for (x, _), w in zip(items, shares)])
        result = (summed / total).astype(BF16)
        for j in range(GROUP):
            at = (g * GROUP + j) * HEAD_SIZE
            picked = []
            for c in range(chains):
                part = result[(c * GROUP + j) * span : (c * GROUP + j + 1) * span, :]
                attended_ref[c, :, pl.ds(at, HEAD_SIZE)] = part
                picked.append(part)
            logits = logits + jnp.dot(
                jnp.concatenate(picked, axis=0),
                w_ref[pl.ds(at, HEAD_SIZE), :],
                preferred_element_type=F32,
            )
    logits_ref[...] = logits


def finish(shape, mine, w_cand, partials):
    chains, span, _ = shape
    return pl.pallas_call(
        functools.partial(finish_kernel, chains, span),
        out_shape=(
            jax.ShapeDtypeStruct(shape, BF16),
            jax.ShapeDtypeStruct((chains * span, NCAND), F32),
        ),
        in_specs=[pl.BlockSpec(memory_space=VMEM)] * (3 + len(partials)),
        out_specs=(pl.BlockSpec(memory_space=VMEM),) * 2,
        compiler_params=params(),
        cost_estimate=pl.CostEstimate(flops=1 << 24, bytes_accessed=1 << 20, transcendentals=0),
    )(*mine, w_cand, *partials)


def score_kernel(answer_ref, gathered_ref, score_ref, tally_ref):
    parts = gathered_ref.shape[0]
    position = lax.axis_index("dp")
    chains = score_ref.shape[0]
    span = gathered_ref.shape[1] // chains
    logits = functools.reduce(lambda a, b: a + b, [gathered_ref[p] for p in range(parts)])
    top = jnp.max(logits, axis=1, keepdims=True)
    norm = top + jnp.log(jnp.sum(jnp.exp(logits - top), axis=1, keepdims=True))
    lane = lax.broadcasted_iota(jnp.int32, (span, NCAND), 1)
    line = lax.broadcasted_iota(jnp.int32, tally_ref.shape, 0)
    column = lax.broadcasted_iota(jnp.int32, tally_ref.shape, 1)
    tally = jnp.zeros(tally_ref.shape, F32)
    for c in range(chains):
        here = slice(c * span, (c + 1) * span)
        chosen = jnp.sum(jnp.where(lane == answer_ref[c], logits[here], 0.0), axis=1, keepdims=True)
        score = jnp.sum(chosen - norm[here], axis=0, keepdims=True) / span
        score_ref[c : c + 1, :] = jnp.broadcast_to(score, (1, NCAND))
        prompt = (position * chains + c) // SAMPLES
        tally = tally + jnp.where((line == prompt) & (column == answer_ref[c]), score, 0.0)
    tally_ref[...] = tally


def score(gathered, answer_id, prompts):
    chains = answer_id.shape[0]
    return pl.pallas_call(
        score_kernel,
        out_shape=(
            jax.ShapeDtypeStruct((chains, NCAND), F32),
            jax.ShapeDtypeStruct((prompts, NCAND), F32),
        ),
        in_specs=[pl.BlockSpec(memory_space=pltpu.SMEM), pl.BlockSpec(memory_space=VMEM)],
        out_specs=(pl.BlockSpec(memory_space=VMEM),) * 2,
        compiler_params=params(8),
        cost_estimate=pl.CostEstimate(flops=1 << 20, bytes_accessed=1 << 16, transcendentals=0),
    )(answer_id, gathered)


def program(queries, key_value_cache, slot_tags, span_key_value, answer_id, w_cand):
    owners = lax.axis_size("dp")
    chains_here = queries.shape[0]
    width = key_value_cache.shape[2]
    teams = owners // TEAM
    others = teams - 1

    def across(array, step):
        pairs = [(((t + step) % teams) * TEAM + r, t * TEAM + r) for t in range(teams) for r in range(TEAM)]
        return lax.ppermute(array, "dp", pairs)

    def within(array, offset):
        return lax.ppermute(array, "dp", [(i, i ^ offset) for i in range(owners)])

    def crosswise(array, step):
        pairs = [
            (((t + step) % teams) * TEAM + (r ^ DIAGONAL), t * TEAM + r) for t in range(teams) for r in range(TEAM)
        ]
        return lax.ppermute(array, "dp", pairs)

    key_value_cache = key_value_cache.reshape(key_value_cache.shape[0], 2 * width, -1)
    slot_tags = pltpu.with_memory_space_constraint(slot_tags, pltpu.HBM)
    key_value_cache = pltpu.with_memory_space_constraint(key_value_cache, pltpu.HBM)
    jobs = [(1, 1, others), (2, 1, others), (0, 1, others), (1, 0, 1), (2, 0, 1), (0, 0, 1), (DIAGONAL, 0, teams)]
    messages = pack(jobs, chains_here, owners, slot_tags, key_value_cache)
    far_in, near_in = [], []
    for j in (1, 2):
        far_in.append(within(messages[j - 1], j))
    visiting = [across(queries, step) for step in range(1, teams)]
    mates = [within(queries, DIAGONAL)]
    mates += [crosswise(queries, step) for step in range(1, teams)]
    for j in (1, 2):
        near_in.append(within(messages[j + 2], j))
    folded = fold(visiting, [messages[2]] + far_in, width)
    partials = [across(m, teams - step) for m, step in zip(folded, range(1, teams))]
    answers = fold(mates, [messages[6]], width)
    partials.append(within(answers[0], DIAGONAL))
    partials += [crosswise(m, teams - step) for m, step in zip(answers[1:], range(1, teams))]
    mine = own(queries, span_key_value, [messages[5]] + near_in, width)
    attended, partial_logits = finish(queries.shape, mine, w_cand, partials)
    gathered = lax.all_gather(partial_logits, "mp")
    prompts = owners * chains_here // SAMPLES
    scores, tally = score(gathered, answer_id, prompts)
    chain_score = scores[:, 0]
    step = 1
    while step < owners:
        tally = tally + within(tally, step)
        step *= 2
    per = NCAND // owners
    answer_tally = lax.dynamic_slice_in_dim(tally, lax.axis_index("dp") * per, per, axis=1)
    return attended, chain_score, answer_tally


def solution(mesh):
    in_specs = (
        P("dp", None, "mp"),
        P("dp", None, None, "mp"),
        P("dp"),
        P("dp", None, None, "mp"),
        P("dp"),
        P("mp", None),
    )
    out_specs = (P("dp", None, "mp"), P("dp"), P(None, "dp"))
    return jax.shard_map(program, mesh=mesh, in_specs=in_specs, out_specs=out_specs, check_vma=False)
```
